32 devices in a mesh: grp: 4 (over y, x), chan: 8 (over z, core).
Axes of the slice: x: 2, y: 2, z: 4, core: 2. Of those that a mesh axis runs over, the one named last changes fastest.
Arguments:
- visibility: float32 [1024, 32768], P('chan', 'grp'), may hold values from -6 to 6
- interference_mask: int32 [1024, 16384], P(None, ('grp', 'chan')), may hold values from 0 to 1
- valid_time_count: int32 [512], P(('grp', 'chan')), may hold values from 8 to 32
- fit_modes: float32 [1024, 32], P('grp'), may hold values from -1 to 1
Outputs:
- residual_vis: float32 [1024, 32768], P('chan', 'grp')
The draws below stay inside these ranges and needn't reach their ends.
All inputs are finite; a program needn't handle non-finite values.
Results may differ from the reference program's by a relative error of at most 0.0003.
Values sent between devices are 32-bit elements; how exact they have to be, the bound alone decides.
A program may use at most 128 MiB of HBM per device.

```python
import jax
import jax.numpy as jnp
from jax import lax

FREQ = 1024
MODES = 32
NT = 32
BASE_DEV = 16
BASE = 512
N_GRP = 4
N_CHAN = 8


def draw_interference_mask(key, part):
    start_key = jax.random.fold_in(key, 11)
    length_key = jax.random.fold_in(key, 12)
    speck_key = jax.random.fold_in(key, 13)
    columns = BASE * NT
    band_start = jax.random.randint(start_key, (1, columns), 0, FREQ, dtype=jnp.int32)
    band_length = jax.random.randint(length_key, (1, columns), 0, FREQ * 7 // 8 + 1, dtype=jnp.int32)
    freq_index = lax.broadcasted_iota(jnp.int32, (FREQ, columns), 0)
    inside_band = (freq_index >= band_start) & (freq_index < band_start + band_length)
    scattered = jax.random.randint(speck_key, (FREQ, columns), 0, 16, dtype=jnp.int32) == 0
    return (inside_band | scattered).astype(jnp.int32)


def draw_fit_modes(key, part):
    center_key = jax.random.fold_in(key, 21)
    rough_key = jax.random.fold_in(key, 22)
    centers = jax.random.uniform(center_key, (1, MODES), jnp.float32, 0.0, 1.0) * FREQ
    freq_index = lax.broadcasted_iota(jnp.float32, (FREQ, MODES), 0)
    spread = FREQ / 6.0
    offset = (freq_index - centers) / spread
    envelope = 0.25 + 1.75 * jnp.exp(-0.5 * offset * offset)
    rough = jnp.clip(jax.random.normal(rough_key, (FREQ, MODES), jnp.float32), -4.0, 4.0)
    column_scale = jnp.sqrt(jnp.sum(envelope * envelope, axis=0, keepdims=True))
    return jnp.clip(rough * envelope / column_scale, -1.0, 1.0)


def plant(values, own_key, least, top_value):
    extent = values.shape
    index_at = [jax.random.randint(jax.random.fold_in(own_key, axis), (), 0, extent[axis]) for axis in range(len(extent))]
    values = values.at[tuple(index_at)].set(least)
    longest = extent.index(max(extent))
    index_at[longest] = (index_at[longest] + 1) % extent[longest]
    return values.at[tuple(index_at)].set(top_value)


def levels(own_key, shape, pieces, smallest, largest):
    level = 1.0
    for dim, parts in pieces:
        heights = jax.random.uniform(jax.random.fold_in(jax.random.fold_in(own_key, 6), dim), (parts,), jnp.float32, smallest / len(pieces), largest / len(pieces))
        level = level * jnp.repeat(jnp.exp(heights), shape[dim] // parts).reshape((-1,) + (1,) * (len(shape) - 1 - dim))
    return level


def noise(stream_key, dims, width, limit, cuts=(), held_as=jnp.bfloat16):
    values = jax.random.normal(stream_key, dims, jnp.float32) * width
    if len(cuts) > 0:
        values = levels(stream_key, dims, cuts, -0.22, 0.18) * values
    return jnp.clip(values, min=-limit, max=limit).astype(held_as)


def setup_inputs(seed: int = 0) -> dict:
    seeds = jax.random.split(jax.random.key(seed), 5)
    return {
        "visibility": noise(seeds[0], (FREQ, BASE * 2 * NT), 1.0, 6.0, ((0, 8), (1, 4)), jnp.float32),
        "interference_mask": draw_interference_mask(jax.random.fold_in(seeds[4], 71), 0),
        "valid_time_count": plant(jax.random.randint(seeds[2], (BASE,), NT // 4, NT + 1), jax.random.fold_in(seeds[2], 1), NT // 4, NT).astype(jnp.int32),
        "fit_modes": draw_fit_modes(jax.random.fold_in(seeds[4], 71), 0),
    }


damping = 0.1

def fit_weight(interference_mask, valid_time_count):
    antenna_pairs_list = valid_time_count.shape[0]
    sample_values = interference_mask.shape[1] // antenna_pairs_list
    projection_sums = lax.broadcasted_iota(jnp.int32, (antenna_pairs_list, sample_values), 1)
    within_range = (projection_sums < valid_time_count[:, None]).astype(jnp.float32).reshape(1, antenna_pairs_list * sample_values)
    return (1.0 - interference_mask.astype(jnp.float32)) * within_range

def solve_normal(normal_matrix, target_signal):
    span_length = normal_matrix.shape[0]
    trailing = normal_matrix
    columns = []
    for position in range(span_length):
        column = trailing[:, 0] / jnp.sqrt(trailing[0, 0])
        columns.append(column)
        trailing = trailing[1:, 1:] - column[1:, None, :] * column[None, 1:, :]
    remains = target_signal
    forward = []
    for position in range(span_length):
        column = columns[position]
        current = remains[0] / column[0][None, :]
        forward.append(current)
        remains = remains[1:] - column[1:, None, :] * current[None]
    solution_values = [None] * span_length
    for position in reversed(range(span_length)):
        column = columns[position]
        current = forward[position]
        if position + 1 < span_length:
            later_rows = jnp.stack(solution_values[position + 1:], 0)
            current = current - lax.optimization_barrier(jnp.sum(column[1:, None, :] * later_rows, axis=0))
        solution_values[position] = current / column[0][None, :]
    return jnp.stack(solution_values, 0)

def solve_amplitudes(spectral_templates, assigned_rows, sample_weight, antenna_pairs_list):
    channel_count, span_length = spectral_templates.shape
    sample_values = sample_weight.shape[1] // antenna_pairs_list
    pairs = (spectral_templates[:, :, None] * spectral_templates[:, None, :]).reshape(channel_count, span_length * span_length)
    normal_matrix = lax.dot_general(pairs, sample_weight, (((0,), (0,)), ((), ())), precision=lax.Precision.HIGHEST, preferred_element_type=jnp.float32)
    normal_matrix = normal_matrix.reshape(span_length, span_length, antenna_pairs_list * sample_values)
    normal_matrix = normal_matrix + damping * jnp.eye(span_length, dtype=normal_matrix.dtype)[:, :, None]
    weighted_values = assigned_rows.reshape(channel_count, antenna_pairs_list, 2, sample_values) * sample_weight.reshape(channel_count, antenna_pairs_list, 1, sample_values)
    weighted_values = weighted_values.reshape(channel_count, antenna_pairs_list * 2 * sample_values)
    template_projection = lax.dot_general(spectral_templates, weighted_values, (((0,), (0,)), ((), ())), precision=lax.Precision.HIGHEST, preferred_element_type=jnp.float32)
    target_signal = template_projection.reshape(span_length, antenna_pairs_list, 2, sample_values).transpose(0, 2, 1, 3).reshape(span_length, 2, antenna_pairs_list * sample_values)
    solution_values = solve_normal(normal_matrix, target_signal)
    return solution_values.reshape(span_length, 2, antenna_pairs_list, sample_values).transpose(0, 2, 1, 3).reshape(span_length, antenna_pairs_list * 2 * sample_values)

def reference(visibility, interference_mask, valid_time_count, fit_modes):
    blocks = N_GRP * N_CHAN
    stacked = visibility.reshape(FREQ, blocks, BASE_DEV * 2 * NT).transpose(1, 0, 2)
    flagged = interference_mask.reshape(FREQ, blocks, BASE_DEV * NT).transpose(1, 0, 2)
    counted = valid_time_count.reshape(blocks, BASE_DEV)

    def one_block(items):
        assigned_rows, block_flags, block_counts = items
        sample_weight = fit_weight(block_flags, block_counts)
        mode_amplitudes = solve_amplitudes(fit_modes, assigned_rows, sample_weight, BASE_DEV)
        model = jnp.dot(fit_modes, mode_amplitudes, precision=lax.Precision.HIGHEST, preferred_element_type=jnp.float32)
        return assigned_rows - model
    result = lax.map(one_block, (stacked, flagged, counted))
    return result.transpose(1, 0, 2).reshape(FREQ, BASE * 2 * NT)
```

```python
import functools
import math

import jax
import jax.numpy as jnp
from jax import lax
from jax.experimental import pallas as pl
from jax.experimental.pallas import tpu as pltpu
from jax.sharding import PartitionSpec as P

damping = 0.1
LANES = 128
VMEM = pl.BlockSpec(memory_space=pltpu.VMEM)
MESH = pl.DeviceIdType.MESH
f32, bf16 = jnp.float32, jnp.bfloat16


def pieces(x):
    hi = x.astype(bf16)
    rest = x - hi.astype(f32)
    mid = rest.astype(bf16)
    return hi, mid, (rest - mid.astype(f32)).astype(bf16)


def factor_kernel(mt_ref, mask_ref, valid, spread, l_ref, inv_ref, w_ref, hi_ref, mid_ref, lo_ref):
    modes, freqs = mt_ref.shape
    columns = mask_ref.shape[1]
    for j in range(columns // LANES):
        part = slice(j * LANES, (j + 1) * LANES)
        w = (1.0 - mask_ref[:, part].astype(f32)) * valid[:, part]
        w_ref[:, 2 * j * LANES : 2 * (j + 1) * LANES] = jnp.dot(
            w.astype(bf16), spread, preferred_element_type=f32
        ).astype(bf16)

    def split(i, carry):
        rows = pl.ds(pl.multiple_of(i * modes, modes), modes)
        hi_ref[rows, :], mid_ref[rows, :], lo_ref[rows, :] = pieces(mt_ref[...] * mt_ref[pl.ds(i, 1), :])
        return carry

    lax.fori_loop(0, modes, split, 0)
    tile, group = 2 * LANES, 8

    def gram(step, carry):
        cols = pl.ds(pl.multiple_of(step // (modes // group) * tile, tile), tile)
        first = step % (modes // group)
        rows = pl.ds(pl.multiple_of(first * group * modes, group * modes), group * modes)
        w = w_ref[:, cols]
        total = jnp.dot(lo_ref[rows, :], w, preferred_element_type=f32)
        total += jnp.dot(mid_ref[rows, :], w, preferred_element_type=f32)
        total += jnp.dot(hi_ref[rows, :], w, preferred_element_type=f32)
        l_ref[pl.ds(first * group, group), :, cols] = total.reshape(group, modes, tile)
        return carry

    lax.fori_loop(0, 2 * columns // tile * (modes // group), gram, 0)
    width = 4 * LANES

    def cholesky(step, carry):
        cols = pl.ds(pl.multiple_of(step * width, width), width)
        for k in range(modes):
            low = k // 8 * 8
            row = lax.broadcasted_iota(jnp.int32, (modes - low, width), 0) + low
            acc = l_ref[k, low:, cols] + jnp.where(row == k, damping, 0.0)
            for m in range(k):
                acc = acc - l_ref[m, low:, cols] * l_ref[m, k : k + 1, cols]
            inv = 1.0 / jnp.sqrt(acc[k - low : k - low + 1])
            inv_ref[k : k + 1, cols] = inv
            l_ref[k, low:, cols] = acc * inv
        return carry

    lax.fori_loop(0, 2 * columns // width, cholesky, 0)


def fit_kernel(chips, groups, vis_hbm, mask_hbm, count_hbm, share_hbm, out_ref,
               vis_ref, own_ref, mask_ref, counts, mt_all, loc_ref, left_ref, w_ref, hi_ref, mid_ref, lo_ref,
               l_ref, inv_ref, give, keep, take, fwd, come, coef,
               pair_sems, fwd_sems, come_sems, near_sems, relay_sems, mate_sems, mask_sems, table_sems, local_sems):
    me, grp = lax.axis_index("chan"), lax.axis_index("grp")
    chip, core = me // 2, me % 2
    pairs = chips // 2
    pair, side = chip // 2, chip % 2
    partner = chip + 1 - 2 * side
    mate = chip * 2 + 1 - core
    turn = 1 - 2 * (2 * chip // chips)
    modes, width = inv_ref.shape
    rows = vis_ref.shape[0]
    chunks, tile = keep.shape[0], keep.shape[3]
    columns = own_ref.shape[1]
    share = share_hbm.shape[1]
    bases = counts.shape[0]
    times = columns // bases

    def other(d):
        return lax.rem(chip + turn * d + chips, chips)

    def toward(slot):
        return jnp.logical_or(jnp.logical_and(slot // 2 > pair, side == 1), jnp.logical_and(slot // 2 < pair, side == 0))

    def nearest(p):
        return jnp.where(p == pair, partner, jnp.where(p > pair, 2 * p, 2 * p + 1))

    load_share = pltpu.make_async_copy(share_hbm, mt_all.at[:, pl.ds(pl.multiple_of(grp * share, share), share)], local_sems.at[3])
    load_share.start()
    load_counts = pltpu.make_async_copy(count_hbm, counts, local_sems.at[4])
    load_counts.start()
    load_own = pltpu.make_async_copy(mask_hbm, own_ref, local_sems.at[0])
    load_own.start()
    barrier = pltpu.get_barrier_semaphore()
    for d in range(1, 2 * chips):
        pl.semaphore_signal(barrier, inc=1, device_id={"chan": lax.rem(me + d, 2 * chips)}, device_id_type=MESH)
    for d in range(1, groups):
        pl.semaphore_signal(barrier, inc=1, device_id={"grp": lax.rem(grp + d, groups)}, device_id_type=MESH)
    pl.semaphore_wait(barrier, 2 * chips + groups - 2)

    def flags(k, peer, slot):
        return pltpu.make_async_remote_copy(
            src_ref=mask_hbm.at[pl.ds(pl.multiple_of(peer * rows, rows), rows), pl.ds(pl.multiple_of(k * LANES, LANES), LANES)],
            dst_ref=mask_ref.at[slot, k], send_sem=mask_sems.at[0, k, peer], recv_sem=mask_sems.at[1, k, slot],
            device_id={"chan": peer}, device_id_type=MESH)

    def modes_copy(peer, slot):
        return pltpu.make_async_remote_copy(
            src_ref=share_hbm, dst_ref=mt_all.at[:, pl.ds(pl.multiple_of(slot * share, share), share)],
            send_sem=table_sems.at[0, peer], recv_sem=table_sems.at[1, slot], device_id={"grp": peer}, device_id_type=MESH)

    def send_flags(k):
        flags(k, mate, me).start()

        def send(d, carry):
            flags(k, other(d) * 2 + core, me).start()
            flags(k, other(d) * 2 + 1 - core, me).start()
            return carry

        lax.fori_loop(1, chips, send, 0)

    ahead = min(2, chunks)
    for d in range(1, groups):
        modes_copy(lax.rem(grp + d, groups), grp).start()
    for k in range(ahead):
        send_flags(k)
    inner = jnp.logical_or(jnp.logical_and(side == 1, pair == 0), jnp.logical_and(side == 0, pair == pairs - 1))

    @pl.when(inner)
    def _():
        for k in range(ahead, chunks):
            send_flags(k)

    load_vis = pltpu.make_async_copy(vis_hbm, vis_ref, local_sems.at[1])
    load_vis.start()

    def load_mine(k):
        return pltpu.make_async_copy(
            mask_hbm.at[pl.ds(pl.multiple_of(me * rows, rows), rows), k * LANES : (k + 1) * LANES],
            mask_ref.at[me, k], local_sems.at[5 + k])

    for k in range(chunks):
        load_mine(k).start()

    source = lax.broadcasted_iota(jnp.int32, (LANES, 2 * LANES), 0)
    column = lax.broadcasted_iota(jnp.int32, (LANES, 2 * LANES), 1)
    spread = jnp.where(source == column // (2 * times) * times + column % times, 1.0, 0.0).astype(bf16)
    load_counts.wait()
    lane = lax.broadcasted_iota(jnp.int32, (1, columns), 1)
    held = jnp.zeros((1, columns), jnp.int32)
    for b in range(bases):
        held = jnp.where(lane // times == b, counts[b], held)
    valid = jnp.where(lane % times < held, 1.0, 0.0)
    lane = lax.broadcasted_iota(jnp.int32, (1, width), 1)
    held = jnp.zeros((1, width), jnp.int32)
    for b in range(bases):
        held = jnp.where(lane // (2 * times) == b, counts[b], held)
    valid_wide = jnp.where(lane % times < held, 1.0, 0.0)

    load_share.wait()
    for d in range(1, groups):
        peer = lax.rem(grp + d, groups)
        modes_copy(peer, peer).wait_recv()
    pick = lax.broadcasted_iota(jnp.int32, (groups * share, rows), 0)
    pick = pick == lax.broadcasted_iota(jnp.int32, (groups * share, rows), 1) + me * rows
    loc = jnp.dot(mt_all[...], pick.astype(f32), precision=lax.Precision.HIGHEST, preferred_element_type=f32)
    loc_ref[...] = loc
    hi, mid, lo = pieces(loc)
    left_ref[...] = jnp.concatenate([hi, hi, mid, mid, hi, lo], axis=0)
    load_own.wait()
    factor_kernel(mt_all, own_ref, valid, spread, l_ref, inv_ref, w_ref, hi_ref, mid_ref, lo_ref)
    load_vis.wait()
    for k in range(chunks):
        load_mine(k).wait()

    def remote(src, dst, send, recv, peer):
        return pltpu.make_async_remote_copy(
            src_ref=src, dst_ref=dst, send_sem=send, recv_sem=recv, device_id={"chan": peer}, device_id_type=MESH)

    def swap(k, slot):
        return remote(give.at[k, slot], take.at[k, slot], pair_sems.at[0, k, slot], pair_sems.at[1, k, slot], mate)

    def pass_on(k, slot):
        return remote(keep.at[k, slot], fwd.at[k, slot], fwd_sems.at[0, k, slot], fwd_sems.at[1, k, slot], partner * 2 + core)

    def deliver(k, slot, at):
        return remote(keep.at[k, slot], come.at[k, at], come_sems.at[0, k, slot], come_sems.at[1, k, at], slot * 2 + core)

    def vis_at(owner, k):
        return pl.ds(pl.multiple_of(owner * width + k * tile, tile), tile)

    def project(owner, k):
        w = 1.0 - mask_ref[owner, k].astype(f32)
        w = jnp.dot(w.astype(bf16), spread, preferred_element_type=f32)
        return jnp.dot(loc_ref[...], vis_ref[:, vis_at(owner, k)] * w,
                       precision=lax.Precision.HIGHEST, preferred_element_type=f32)

    def near_pair(slot):
        return jnp.logical_and(slot // 2 == pair, slot != chip)

    def passed(slot):
        return jnp.logical_and(slot // 2 != pair, jnp.logical_not(toward(slot)))

    def chunk(k, carry):
        def partial(d, c):
            slot = other(d)
            first, second = slot * 2 + 1 - core, slot * 2 + core
            flags(k, first, first).wait_recv()
            give[k, slot] = project(first, k)
            swap(k, slot).start()

            @pl.when(d > 0)
            def _():
                flags(k, second, second).wait_recv()

            keep[k, slot] = project(second, k)
            return c

        lax.fori_loop(0, chips, partial, 0)

        def merge(d, c):
            slot = other(d)
            swap(k, slot).wait()
            keep[k, slot] = keep[k, slot] + take[k, slot]

            @pl.when(near_pair(slot))
            def _():
                deliver(k, slot, pair).start()

            @pl.when(passed(slot))
            def _():
                pass_on(k, slot).start()

            return c

        lax.fori_loop(0, chips, merge, 0)

        @pl.when(jnp.logical_and(jnp.logical_not(inner), k + ahead < chunks))
        def _():
            send_flags(k + ahead)

        @pl.when(k > 0)
        def _():
            join(k - 1)

        return carry

    def join(k):
        def step(d, c):
            slot = other(d)

            @pl.when(toward(slot))
            def _():
                pass_on(k, slot).wait_recv()
                keep[k, slot] = keep[k, slot] + fwd[k, slot]
                deliver(k, slot, pair).start()

            return c

        lax.fori_loop(1, chips, step, 0)

    lax.fori_loop(0, chunks, chunk, 0)
    join(chunks - 1)

    def near(k, p):
        block = coef.at[k, me]
        peer = nearest(p)
        return remote(block, block, near_sems.at[0, k, p], near_sems.at[1, k, chip], peer * 2 + core)

    def arrived(k, slot):
        block = coef.at[k, slot * 2 + core]
        return remote(block, block, near_sems.at[0, k, 0], near_sems.at[1, k, slot], slot * 2 + core)

    def relay(k, slot):
        block = coef.at[k, slot * 2 + core]
        return remote(block, block, relay_sems.at[k, slot], near_sems.at[1, k, slot], partner * 2 + core)

    def to_mate(k, slot):
        block = coef.at[k, slot * 2 + core]
        return remote(block, block, mate_sems.at[0, k, slot], mate_sems.at[1, k, slot], mate)

    def from_mate(k, slot):
        block = coef.at[k, slot * 2 + 1 - core]
        return remote(block, block, mate_sems.at[0, k, slot], mate_sems.at[1, k, slot], mate)

    def solve(k):
        total = keep[k, chip]
        for p in range(pairs):
            deliver(k, chip, p).wait_recv()
            total = total + come[k, p]
        cols = pl.ds(k * tile, tile)
        left = total * valid_wide[:, k * tile : (k + 1) * tile]
        parts = [left[g * 8 : (g + 1) * 8] for g in range(modes // 8)]
        ys = []
        for m in range(modes):
            low = m // 8
            y = parts[low][m % 8 : m % 8 + 1] * inv_ref[m : m + 1, cols]
            ys.append(y)
            for g in range(low, modes // 8):
                parts[g] = parts[g] - l_ref[m, g * 8 : (g + 1) * 8, cols] * y
        row = lax.broadcasted_iota(jnp.int32, (8, tile), 0)
        xs = [jnp.zeros((8, tile), f32) for _ in range(modes // 8)]
        for m in reversed(range(modes)):
            low = m // 8
            acc = l_ref[m, low * 8 : (low + 1) * 8, cols] * xs[low]
            for g in range(low + 1, modes // 8):
                acc = acc + l_ref[m, g * 8 : (g + 1) * 8, cols] * xs[g]
            x = (ys[m] - jnp.sum(acc, axis=0, keepdims=True)) * inv_ref[m : m + 1, cols]
            xs[low] = jnp.where(row == m % 8, x, xs[low])
        for g in range(modes // 8):
            coef[k, me, g * 8 : (g + 1) * 8, :] = xs[g]
        for p in range(pairs):
            near(k, p).start()
        to_mate(k, chip).start()

    def spread_coef(k):
        def step(d, c):
            slot = other(d)
            arrived(k, slot).wait_recv()

            @pl.when(toward(slot))
            def _():
                relay(k, slot).start()

            to_mate(k, slot).start()
            return c

        lax.fori_loop(1, chips, step, 0)

    def subtract(owner, k):
        hi, mid, lo = pieces(coef[k, owner])
        right = jnp.concatenate([hi, mid, hi, mid, lo, hi], axis=0)
        cols = vis_at(owner, k)
        out_ref[:, cols] = vis_ref[:, cols] - lax.dot_general(
            left_ref[...], right, (((0,), (0,)), ((), ())), preferred_element_type=f32)

    def residual(k):
        def step(d, c):
            slot = other(d)
            subtract(slot * 2 + core, k)
            from_mate(k, slot).wait_recv()
            subtract(slot * 2 + 1 - core, k)
            return c

        lax.fori_loop(0, chips, step, 0)

    for k in range(chunks):
        solve(k)
        if k > 0:
            spread_coef(k - 1)
            residual(k - 1)
    spread_coef(chunks - 1)
    residual(chunks - 1)

    def finish(k, carry):
        flags(k, mate, me).wait_send()
        for p in range(pairs):
            near(k, p).wait_send()

        def step(d, c):
            slot = other(d)
            to_mate(k, slot).wait_send()

            @pl.when(d > 0)
            def _():
                flags(k, slot * 2 + core, me).wait_send()
                flags(k, slot * 2 + 1 - core, me).wait_send()

            @pl.when(passed(slot))
            def _():
                pass_on(k, slot).wait_send()

            @pl.when(jnp.logical_or(near_pair(slot), toward(slot)))
            def _():
                deliver(k, slot, pair).wait_send()

            @pl.when(toward(slot))
            def _():
                relay(k, slot).wait_send()

            return c

        lax.fori_loop(0, chips, step, 0)
        return carry

    lax.fori_loop(0, chunks, finish, 0)
    for d in range(1, groups):
        modes_copy(lax.rem(grp + d, groups), grp).wait_send()


def per_device(chan, groups, visibility, interference_mask, valid_time_count, fit_modes):
    rows, all_columns = visibility.shape
    freqs, columns = interference_mask.shape
    share, modes = fit_modes.shape
    bases = valid_time_count.shape[0]
    width = 2 * columns
    chips = chan // 2
    chunks, tile = columns // LANES, 2 * LANES
    block = pltpu.VMEM((chunks, chips, modes, tile), f32)
    anywhere = pl.BlockSpec(memory_space=pltpu.HBM)
    dma = pltpu.SemaphoreType.DMA
    scratch = (
        [
            pltpu.VMEM((rows, all_columns), f32),
            pltpu.VMEM((freqs, columns), jnp.int32),
            pltpu.VMEM((chan, chunks, rows, LANES), jnp.int32),
            pltpu.SMEM((bases,), jnp.int32),
            pltpu.VMEM((modes, freqs), f32),
            pltpu.VMEM((modes, rows), f32),
            pltpu.VMEM((6 * modes, rows), bf16),
            pltpu.VMEM((freqs, width), bf16),
        ]
        + [pltpu.VMEM((modes * modes, freqs), bf16)] * 3
        + [pltpu.VMEM((modes, modes, width), f32), pltpu.VMEM((modes, width), f32)]
        + [block] * 4
        + [pltpu.VMEM((chunks, chips // 2, modes, tile), f32), pltpu.VMEM((chunks, chan, modes, tile), f32)]
        + [dma((2, chunks, chips))] * 3
        + [dma((2, chunks, chips)), dma((chunks, chips)), dma((2, chunks, chips)), dma((2, chunks, chan)),
           dma((2, groups)), dma((5 + chunks,))]
    )
    held = sum(math.prod(s.shape) * jnp.dtype(s.dtype).itemsize for s in scratch[:-9])
    return pl.pallas_call(
        functools.partial(fit_kernel, chips, groups),
        out_shape=jax.ShapeDtypeStruct((rows, all_columns), f32),
        in_specs=[anywhere] * 4,
        out_specs=VMEM,
        scratch_shapes=scratch,
        compiler_params=pltpu.CompilerParams(
            collective_id=0, has_side_effects=True, vmem_limit_bytes=held + (5 << 20)),
        cost_estimate=pl.CostEstimate(flops=10**10, bytes_accessed=12 << 20, transcendentals=0),
        name="fit",
    )(*[pltpu.with_memory_space_constraint(a, pltpu.HBM)
        for a in (visibility, interference_mask, valid_time_count, fit_modes.T)])


def solution(mesh):
    placed = (P("chan", "grp"), P(None, ("grp", "chan")), P(("grp", "chan")), P("grp", None))
    return jax.shard_map(
        functools.partial(per_device, mesh.shape["chan"], mesh.shape["grp"]), mesh=mesh, in_specs=placed,
        out_specs=P("chan", "grp"), check_vma=False)
```
